32 devices in a mesh: row: 8 (over z, x), col: 4 (over y, core).
Axes of the slice: x: 2, y: 2, z: 4, core: 2. Of those that a mesh axis runs over, the one named last changes fastest.
Arguments:
- homolog_stack: float32 [16, 64, 64], P(None, ('row', 'col')), may hold values from -6 to 6
- residue_grid: float32 [64, 64, 128], P('row', 'col'), may hold values from -6 to 27
- first_tensor_matrix: float32 [64, 32], replicated, may hold values from -0.75 to 0.75
- second_tensor_matrix: float32 [64, 32], replicated, may hold values from -0.75 to 0.75
- tensor_flatten_matrix: float32 [1024, 128], replicated, may hold values from -0.1875 to 0.1875
- tensor_offset_vector: float32 [128], replicated, may hold values from -3 to 3
- feedforward_switch_matrix: float32 [128, 512], replicated, may hold values from -0.5 to 0.5
- expand_matrix: float32 [128, 512], replicated, may hold values from -0.5 to 0.5
- shrink_matrix: float32 [512, 128], replicated, may hold values from -0.25 to 0.25
- grid_score_matrix: float32 [128, 8], replicated, may hold values from -48 to 48
- homolog_content_matrix: float32 [64, 256], replicated, may hold values from -0.75 to 0.75
- homolog_sigmoid_matrix: float32 [64, 256], replicated, may hold values from -0.75 to 0.75
- mixing_result_matrix: float32 [256, 64], replicated, may hold values from -0.375 to 0.375
Outputs:
- pair_output: float32 [64, 64, 128], P('row', 'col')
- homolog_refreshed: float32 [16, 64, 64], P(None, ('row', 'col'))
The draws below stay inside these ranges and needn't reach their ends.
All inputs are finite; a program needn't handle non-finite values.
Results may differ from the reference program's by a relative error of at most 0.00029.
Values sent between devices are 32-bit elements; how exact they have to be, the bound alone decides.
A program may use at most 64 MiB of HBM per device.

```python
import math
import jax
import jax.numpy as jnp
from jax import lax

HOMOLOG_FEATURES = 64
CZ = 128
PROJECTED_DIMS = 32
FFZ = 512
ATTENTION_GROUPS = 8
GROUP_FEATURES = 32
HOMOLOG_NUMBER = 16
RESIDUE_NUMBER = 64


def draw_grid_score_matrix(key, part):
    noise = jnp.clip(jax.random.normal(jax.random.fold_in(key, 11), (CZ, ATTENTION_GROUPS), jnp.float32), -6.0, 6.0)
    return noise * (3.0 / math.sqrt(CZ))


def draw_residue_grid(key, part):
    base_draw = jnp.clip(jax.random.normal(jax.random.fold_in(key, 13), (RESIDUE_NUMBER, RESIDUE_NUMBER, CZ), jnp.float32), -6.0, 6.0)
    return base_draw


def block_levels(stream_key, dims, split, least, top_value):
    def one(position, shards_of):
        draws = jax.random.uniform(jax.random.fold_in(jax.random.fold_in(stream_key, 6), position), (shards_of,), jnp.float32, least / len(split), top_value / len(split))
        return jnp.repeat(jnp.exp(draws), dims[position] // shards_of).reshape((-1,) + (1,) * (len(dims) - position - 1))

    loudness = one(*split[0])
    for cut in split[1:]:
        loudness = loudness * one(*cut)
    return loudness


def normal_values(rng, extent, width, bound, split=(), kind=jnp.bfloat16):
    values = jax.random.normal(rng, extent, jnp.float32) * width
    if len(split) > 0:
        values = block_levels(rng, extent, split, -0.22, 0.18) * values
    return jnp.clip(values, min=-bound, max=bound).astype(kind)


def setup_inputs(seed: int = 0) -> dict:
    keys = jax.random.split(jax.random.key(seed), 14)
    homolog_stack = normal_values(keys[0], (HOMOLOG_NUMBER, RESIDUE_NUMBER, HOMOLOG_FEATURES), 1.0, 6.0, ((1, 32),), jnp.float32)
    residue_grid = draw_residue_grid(jax.random.fold_in(keys[13], 71), 0)
    first_tensor_matrix = normal_values(keys[2], (HOMOLOG_FEATURES, PROJECTED_DIMS), HOMOLOG_FEATURES ** -0.5, 0.75, (), jnp.float32)
    second_tensor_matrix = normal_values(keys[3], (HOMOLOG_FEATURES, PROJECTED_DIMS), HOMOLOG_FEATURES ** -0.5, 0.75, (), jnp.float32)
    tensor_flatten_matrix = normal_values(keys[4], (PROJECTED_DIMS * PROJECTED_DIMS, CZ), (PROJECTED_DIMS * PROJECTED_DIMS) ** -0.5, 0.1875, (), jnp.float32)
    tensor_offset_vector = normal_values(keys[5], (CZ,), 0.5, 3.0, (), jnp.float32)
    feedforward_switch_matrix = normal_values(keys[6], (CZ, FFZ), CZ ** -0.5, 0.5, (), jnp.float32)
    expand_matrix = normal_values(keys[7], (CZ, FFZ), CZ ** -0.5, 0.5, (), jnp.float32)
    shrink_matrix = normal_values(keys[8], (FFZ, CZ), FFZ ** -0.5, 0.25, (), jnp.float32)
    grid_score_matrix = draw_grid_score_matrix(jax.random.fold_in(keys[13], 71), 0)
    homolog_content_matrix = normal_values(keys[10], (HOMOLOG_FEATURES, ATTENTION_GROUPS * GROUP_FEATURES), HOMOLOG_FEATURES ** -0.5, 0.75, (), jnp.float32)
    homolog_sigmoid_matrix = normal_values(keys[11], (HOMOLOG_FEATURES, ATTENTION_GROUPS * GROUP_FEATURES), HOMOLOG_FEATURES ** -0.5, 0.75, (), jnp.float32)
    mixing_result_matrix = normal_values(keys[12], (ATTENTION_GROUPS * GROUP_FEATURES, HOMOLOG_FEATURES), (ATTENTION_GROUPS * GROUP_FEATURES) ** -0.5, 0.375, (), jnp.float32)
    return {"homolog_stack": homolog_stack, "residue_grid": residue_grid, "first_tensor_matrix": first_tensor_matrix, "second_tensor_matrix": second_tensor_matrix, "tensor_flatten_matrix": tensor_flatten_matrix, "tensor_offset_vector": tensor_offset_vector, "feedforward_switch_matrix": feedforward_switch_matrix, "expand_matrix": expand_matrix, "shrink_matrix": shrink_matrix, "grid_score_matrix": grid_score_matrix, "homolog_content_matrix": homolog_content_matrix, "homolog_sigmoid_matrix": homolog_sigmoid_matrix, "mixing_result_matrix": mixing_result_matrix}


epsilon = 1e-05
exact_matmul_mode = lax.Precision.HIGHEST

def standardize_features(inputs):
    row_mean = lax.optimization_barrier(jnp.mean(inputs, axis=-1, keepdims=True))
    centered = inputs - row_mean
    row_var = lax.optimization_barrier(jnp.mean(centered * centered, axis=-1, keepdims=True))
    return centered * lax.rsqrt(row_var + epsilon)

def reference(homolog_stack, residue_grid, first_tensor_matrix, second_tensor_matrix, tensor_flatten_matrix, tensor_offset_vector, feedforward_switch_matrix, expand_matrix, shrink_matrix, grid_score_matrix, homolog_content_matrix, homolog_sigmoid_matrix, mixing_result_matrix):
    homolog_number = homolog_stack.shape[0]
    homolog_standardized = standardize_features(homolog_stack)
    outer_left_factor = jnp.einsum('eov,vh->eoh', homolog_standardized, first_tensor_matrix, precision=exact_matmul_mode)
    outer_right_factor = jnp.einsum('eov,vh->eoh', homolog_standardized, second_tensor_matrix, precision=exact_matmul_mode)
    value_rows = jnp.einsum('rxv,vy->rxy', homolog_standardized, homolog_content_matrix, precision=exact_matmul_mode)
    block_rows = 32

    def rows_step(row_start):
        left_rows = lax.dynamic_slice_in_dim(outer_left_factor, row_start, block_rows, 1)
        outer_product = jnp.einsum('sic,sjd->ijcd', left_rows, outer_right_factor, precision=exact_matmul_mode) / homolog_number
        outer_product = outer_product.reshape(block_rows, RESIDUE_NUMBER, PROJECTED_DIMS * PROJECTED_DIMS)
        update = jnp.einsum('ijk,kz->ijz', outer_product, tensor_flatten_matrix, precision=exact_matmul_mode) + tensor_offset_vector
        pair_mid = lax.dynamic_slice_in_dim(residue_grid, row_start, block_rows, 0) + update
        normed = standardize_features(pair_mid)
        gate_part = jnp.einsum('ijz,zf->ijf', normed, feedforward_switch_matrix, precision=exact_matmul_mode)
        up_part = jnp.einsum('ijz,zf->ijf', normed, expand_matrix, precision=exact_matmul_mode)
        hidden = jax.nn.silu(gate_part) * up_part
        pair_new = pair_mid + jnp.einsum('ijf,fz->ijz', hidden, shrink_matrix, precision=exact_matmul_mode)
        logits = jnp.einsum('ijz,zh->ijh', standardize_features(pair_new), grid_score_matrix, precision=exact_matmul_mode)
        return (pair_new, logits)
    starts = jnp.arange(RESIDUE_NUMBER // block_rows, dtype=jnp.int32) * block_rows
    pair_blocks, logit_blocks = lax.map(rows_step, starts)
    pair_output = pair_blocks.reshape(RESIDUE_NUMBER, RESIDUE_NUMBER, CZ)
    logits = logit_blocks.reshape(RESIDUE_NUMBER, RESIDUE_NUMBER, ATTENTION_GROUPS)
    weights = jax.nn.softmax(logits, axis=1)
    head_values = value_rows.reshape(homolog_number, RESIDUE_NUMBER, ATTENTION_GROUPS, GROUP_FEATURES)
    grid_mixed = jnp.einsum('ijh,sjhc->sihc', weights, head_values, precision=exact_matmul_mode)
    grid_mixed = grid_mixed.reshape(homolog_number, RESIDUE_NUMBER, ATTENTION_GROUPS * GROUP_FEATURES)
    sigmoid_scores = jax.nn.sigmoid(jnp.einsum('rxv,vy->rxy', homolog_standardized, homolog_sigmoid_matrix, precision=exact_matmul_mode))
    homolog_refreshed = homolog_stack + jnp.einsum('lmx,xy->lmy', sigmoid_scores * grid_mixed, mixing_result_matrix, precision=exact_matmul_mode)
    return (pair_output, homolog_refreshed)
```

```python
import functools

import jax
import jax.numpy as jnp
from jax import lax
from jax.experimental import pallas as pl
from jax.experimental.pallas import tpu as pltpu
from jax.sharding import PartitionSpec as P

epsilon = 1e-05
MESH = pl.DeviceIdType.MESH
f32 = jnp.float32
bf16 = jnp.bfloat16


def split(x):
    hi = x.astype(bf16)
    return hi, (x - hi.astype(f32)).astype(bf16)


def mm(a, b):
    return jnp.dot(a, b, preferred_element_type=f32)


def standardize(x):
    centered = x - jnp.mean(x, axis=-1, keepdims=True)
    return centered * lax.rsqrt(jnp.mean(centered * centered, axis=-1, keepdims=True) + epsilon)


def stacked(x):
    hi, lo = split(x)
    return jnp.concatenate([hi, lo, hi], axis=1)


def stacked_rows(w):
    hi, lo = split(w)
    return jnp.concatenate([hi, hi, lo], axis=0)


def kernel(dims, *refs):
    (R, C, S, TP, I, J, IB) = dims
    (x_h, res_h, fst_h, snd_h, flat_h, off_h, sw_h, ex_h, sh_h, gs_h, ct_h, sg_h, mx_h) = refs[:13]
    (pair_h, hom_o) = refs[13:15]
    (x, res, fst, snd, flat, off, sw, ex, sh, gs, ct, sg, mx) = refs[15:28]
    (rowbuf, colbuf, frep, srep, cstk, wf, wg_hh, wg_l, wsh, grep, mstk, l2, r2, vals, ohl, w2,
     pair, part, got, wide, mixbuf, in_sem, send_sem, row_sem, col_sem, psend, precv, out_sem) = refs[28:]
    r, c = lax.axis_index("row"), lax.axis_index("col")
    lin = r * C + c
    B = S * TP
    CD = flat.shape[0]
    D = fst.shape[1]
    HC = ct.shape[1]
    H = gs.shape[1]
    Z = flat.shape[1]
    FF = sw.shape[1]
    F = fst.shape[0]

    barrier = pltpu.get_barrier_semaphore()
    c_dst = lin // R
    slot = lax.rem(lin, R)
    own = c_dst == c

    def greet(a, b):
        pl.semaphore_signal(barrier, inc=1, device_id=(a, b), device_id_type=MESH)

    copies = []
    for n, (src, dst) in enumerate(zip(
        (x_h, fst_h, snd_h, ct_h, sg_h, gs_h, flat_h, off_h, res_h, sw_h, ex_h, sh_h, mx_h),
        (x, fst, snd, ct, sg, gs, flat, off, res, sw, ex, sh, mx))):
        cp = pltpu.make_async_copy(src, dst, in_sem.at[n])
        cp.start()
        copies.append(cp)
    (cx, cfst, csnd, cct, csg, cgs, cflat, coff, cres, csw, cex, csh, cmx) = copies

    for k in range(1, C):
        greet(r, lax.rem(c + k, C))
    for k in range(1, R):
        greet(lax.rem(r + k, R), c_dst)

    @pl.when(jnp.logical_not(own))
    def _():
        greet(r, c_dst)

    for k in range(R):
        src = c * R + k

        @pl.when(src != lin)
        def _():
            greet(src // C, lax.rem(src, C))

    self_in = jnp.where(own, 1, 0)
    cx.wait()
    pl.semaphore_wait(barrier, (C - 1) + 2 * (R - self_in))

    def row_copy(to, at, n):
        return pltpu.make_async_remote_copy(
            src_ref=x, dst_ref=rowbuf.at[pl.ds(pl.multiple_of(at * B, B), B)],
            send_sem=send_sem.at[n], recv_sem=row_sem.at[at],
            device_id=(r, to), device_id_type=MESH)

    def col_copy(to, at, n):
        return pltpu.make_async_remote_copy(
            src_ref=x, dst_ref=colbuf.at[pl.ds(pl.multiple_of(at * B, B), B)],
            send_sem=send_sem.at[n], recv_sem=col_sem.at[at],
            device_id=(to, c_dst), device_id_type=MESH)

    for k in range(1, R):
        col_copy(lax.rem(r + k, R), slot, C + k).start()

    @pl.when(jnp.logical_not(own))
    def _():
        col_copy(r, slot, C).start()

    for k in range(1, C):
        row_copy(lax.rem(c + k, C), c, k).start()

    mine = x[...]
    rowbuf[pl.ds(pl.multiple_of(c * B, B), B), :] = mine

    @pl.when(own)
    def _():
        colbuf[pl.ds(pl.multiple_of(slot * B, B), B), :] = mine

    lane = lax.broadcasted_iota(jnp.int32, (D, CD), 1)
    sub = lax.broadcasted_iota(jnp.int32, (D, CD), 0)
    rep_of = jnp.where(lane // D == sub, 1.0, 0.0).astype(bf16)
    tile_of = jnp.where(lax.rem(lane, D) == sub, 1.0, 0.0).astype(bf16)
    for cp, w, e, out in ((cfst, fst, rep_of, frep), (csnd, snd, tile_of, srep)):
        cp.wait()
        hi, lo = split(w[...])
        hi = mm(hi, e).astype(bf16)
        out[0:F, :] = hi
        out[F:2 * F, :] = hi
        out[2 * F:3 * F, :] = mm(lo, e).astype(bf16)
    cct.wait()
    cstk[...] = stacked_rows(ct[...])
    cgs.wait()
    head = lax.broadcasted_iota(jnp.int32, (H, HC), 1) // (HC // H)
    spread = jnp.where(head == lax.broadcasted_iota(jnp.int32, (H, HC), 0), 1.0, 0.0).astype(f32)
    grep[...] = jnp.dot(gs[...], spread, precision=lax.Precision.HIGHEST, preferred_element_type=f32)
    cflat.wait()
    hi, lo = split(flat[...])
    wf[:, 0:Z] = hi
    wf[:, Z:2 * Z] = lo
    for cp, w, at in ((csw, sw, 0), (cex, ex, FF)):
        cp.wait()
        hi, lo = split(w[...])
        wg_hh[0:Z, at:at + FF] = hi
        wg_hh[Z:2 * Z, at:at + FF] = hi
        wg_l[:, at:at + FF] = lo
    csh.wait()
    hi, lo = split(sh[...])
    wsh[:, 0:Z] = hi
    wsh[:, Z:2 * Z] = lo
    cmx.wait()
    mstk[...] = stacked_rows(mx[...])
    csg.wait()
    gate = jax.nn.sigmoid(mm(stacked(standardize(mine)), stacked_rows(sg[...])))

    for k in range(C):
        @pl.when(k != c)
        def _():
            row_copy(c, k, 0).wait_recv()
    l2[...] = mm(stacked(standardize(rowbuf[...])), frep[...]) * (1.0 / S)
    for k in range(R):
        @pl.when(c * R + k != lin)
        def _():
            col_copy(r, k, 0).wait_recv()
    cols = standardize(colbuf[...])
    wide[...] = jnp.concatenate([cols, jnp.zeros((R * B, wide.shape[1] - F), f32)], axis=1)
    cols = jnp.concatenate(
        [wide[pl.ds(s * TP + t, R, stride=B), :] for s in range(S) for t in range(TP)], axis=0)
    cols = stacked(cols[:, 0:F])
    r2[...] = mm(cols, srep[...])
    values = mm(cols, cstk[...])
    for h in range(HC // 128):
        vals[h] = values[:, h * 128:(h + 1) * 128]
    coff.wait()
    cres.wait()

    NP = IB * J

    def chunk(i0):
        if I == IB:
            l2c, resc, pairc = l2, res, pair
        else:
            l2c = l2.at[pl.ds(pl.multiple_of((i0 // TP) * B, B), (IB // TP) * B)]
            rows = pl.ds(pl.multiple_of(i0 * J, IB * J), IB * J)
            resc, pairc = res.at[rows], pair.at[rows]

        def lanes_step(lt, carry):
            at = pl.ds(pl.multiple_of(lt * 128, 128), 128)
            acc = [None] * IB
            for s in range(S):
                right = r2[s * J:(s + 1) * J, at]
                for ii in range(IB):
                    left = l2c[pl.ds((ii // TP) * B + s * TP + ii % TP, 1), at]
                    term = left * right
                    acc[ii] = term if s == 0 else acc[ii] + term
            for ii in range(IB):
                hi, lo = split(acc[ii])
                ohl[ii * J:(ii + 1) * J, at] = hi
                ohl[NP + ii * J:NP + (ii + 1) * J, at] = lo
            return carry

        lax.fori_loop(0, CD // 128, lanes_step, 0)
        up = mm(ohl[...], wf[...])
        update = up[0:NP, 0:Z] + (up[NP:, 0:Z] + up[0:NP, Z:])
        base = jnp.concatenate(
            [resc[pl.ds(ii * J + t, R, stride=TP), :] for ii in range(IB) for t in range(TP)], axis=0)
        mid = base + (update + off[...])
        hi, lo = split(standardize(mid))
        hid = mm(jnp.concatenate([hi, lo], axis=1), wg_hh[...]) + mm(hi, wg_l[...])
        g = hid[:, 0:FF]
        hidden = g / (1.0 + jnp.exp(-g)) * hid[:, FF:]
        hi, lo = split(hidden)
        down = mm(jnp.concatenate([hi, lo], axis=0), wsh[...])
        new = mid + (down[0:NP, 0:Z] + (down[NP:, 0:Z] + down[0:NP, Z:]))
        for ii in range(IB):
            for t in range(TP):
                a = (ii * TP + t) * R
                pairc[pl.ds(ii * J + t, R, stride=TP), :] = new[a:a + R, :]
        logits = jnp.dot(standardize(new), grep[...], precision=lax.Precision.HIGHEST,
                         preferred_element_type=f32)
        for ii in range(IB):
            i = i0 + ii
            row = logits[ii * J:(ii + 1) * J, :]
            peak = jnp.max(row, axis=0, keepdims=True)
            e = jnp.exp(row - peak)
            w2[ii * J:(ii + 1) * J, :] = e
            total = jnp.sum(e, axis=0, keepdims=True)
            which = lax.broadcasted_iota(jnp.int32, (8, HC), 0)
            part[i, S:S + 8, :] = jnp.where(which == 0, total, peak)
        for ii in range(IB):
            for h in range(HC // 128):
                at = slice(h * 128, (h + 1) * 128)
                acc = None
                for j in range(J):
                    term = w2[pl.ds(ii * J + j, 1), at] * vals[h, pl.ds(j, S, stride=J), :]
                    acc = term if acc is None else acc + term
                part[i0 + ii, 0:S, at] = acc

    if I == IB:
        chunk(0)
    else:
        def step(n, carry):
            chunk(n * IB)
            return carry
        lax.fori_loop(0, I // IB, step, 0)

    def part_copy(to, at, n):
        return pltpu.make_async_remote_copy(
            src_ref=part.at[pl.ds(to * TP, TP)], dst_ref=got.at[pl.ds(at * TP, TP)],
            send_sem=psend.at[n], recv_sem=precv.at[at],
            device_id=(r, to), device_id_type=MESH)

    for k in range(1, C):
        part_copy(lax.rem(c + k, C), c, k).start()
    out = pltpu.make_async_copy(pair, pair_h, out_sem)
    out.start()
    got[pl.ds(c * TP, TP)] = part[pl.ds(c * TP, TP)]

    for k in range(1, R):
        col_copy(lax.rem(r + k, R), slot, C + k).wait_send()

    @pl.when(jnp.logical_not(own))
    def _():
        col_copy(r, slot, C).wait_send()

    for k in range(1, C):
        row_copy(lax.rem(c + k, C), c, k).wait_send()

    for k in range(C):
        @pl.when(k != c)
        def _():
            part_copy(c, k, 0).wait_recv()

    for t in range(TP):
        peaks = [got[k * TP + t, S + 1:S + 2, :] for k in range(C)]
        top = functools.reduce(jnp.maximum, peaks)
        scale = [jnp.exp(p - top) for p in peaks]
        total = sum(got[k * TP + t, S:S + 1, :] * scale[k] for k in range(C))
        summed = sum(got[k * TP + t, 0:S, :] * scale[k] for k in range(C))
        summed = summed / total
        for h in range(HC // 128):
            mixbuf[h, pl.ds(t, S, stride=TP), :] = summed[:, h * 128:(h + 1) * 128]
    mixed = gate * jnp.concatenate([mixbuf[h] for h in range(HC // 128)], axis=1)
    hom_o[...] = x[...] + mm(stacked(mixed), mstk[...])
    for k in range(1, C):
        part_copy(lax.rem(c + k, C), c, k).wait_send()
    out.wait()


def on_device(R, C, homolog_stack, residue_grid, first, second, flatten, offset, switch, expand,
              shrink, score, content, sig, mixing):
    S, TP, F = homolog_stack.shape
    I, J, Z = residue_grid.shape
    IB = max(TP, min(I, 128 // J))
    NP = IB * J
    CD = flatten.shape[0]
    FF = switch.shape[1]
    HC = content.shape[1]
    B = S * TP
    args = (homolog_stack.reshape(B, F), residue_grid.reshape(I * J, Z), first, second, flatten,
            offset.reshape(1, Z), switch, expand, shrink, score, content, sig, mixing)
    dma = pltpu.SemaphoreType.DMA
    pair, hom = pl.pallas_call(
        functools.partial(kernel, (R, C, S, TP, I, J, IB)),
        out_shape=(jax.ShapeDtypeStruct((I * J, Z), f32), jax.ShapeDtypeStruct((B, F), f32)),
        in_specs=[pl.BlockSpec(memory_space=pl.ANY)] * 13,
        out_specs=(pl.BlockSpec(memory_space=pl.ANY), pl.BlockSpec(memory_space=pltpu.VMEM)),
        scratch_shapes=[pltpu.VMEM(a.shape, f32) for a in args] + [
            pltpu.VMEM((C * B, F), f32),
            pltpu.VMEM((R * B, F), f32),
            pltpu.VMEM((3 * F, CD), bf16),
            pltpu.VMEM((3 * F, CD), bf16),
            pltpu.VMEM((3 * F, HC), bf16),
            pltpu.VMEM((CD, 2 * Z), bf16),
            pltpu.VMEM((2 * Z, 2 * FF), bf16),
            pltpu.VMEM((Z, 2 * FF), bf16),
            pltpu.VMEM((FF, 2 * Z), bf16),
            pltpu.VMEM((Z, HC), f32),
            pltpu.VMEM((3 * HC, F), bf16),
            pltpu.VMEM((C * B, CD), f32),
            pltpu.VMEM((S * J, CD), f32),
            pltpu.VMEM((HC // 128, S * J, 128), f32),
            pltpu.VMEM((2 * NP, CD), bf16),
            pltpu.VMEM((NP, HC), f32),
            pltpu.VMEM((I * J, Z), f32),
            pltpu.VMEM((I, S + 8, HC), f32),
            pltpu.VMEM((I, S + 8, HC), f32),
            pltpu.VMEM((R * B, 128), f32),
            pltpu.VMEM((HC // 128, B, 128), f32),
            dma((13,)), dma((C + R,)), dma((C,)), dma((R,)), dma((C,)), dma((C,)), dma(()),
        ],
        compiler_params=pltpu.CompilerParams(
            collective_id=0, has_side_effects=True, vmem_limit_bytes=60000 * 1024),
        name="msa_block",
    )(*args)
    return pair.reshape(I, J, Z), hom.reshape(S, TP, F)


def solution(mesh):
    R, C = mesh.shape["row"], mesh.shape["col"]
    return jax.shard_map(
        functools.partial(on_device, R, C),
        mesh=mesh,
        in_specs=(P(None, ("row", "col"), None), P("row", "col", None)) + (P(),) * 11,
        out_specs=(P("row", "col", None), P(None, ("row", "col"), None)),
        check_vma=False,
    )
```

```python
import functools

import jax
import jax.numpy as jnp
from jax import lax
from jax.experimental import pallas as pl
from jax.experimental.pallas import tpu as pltpu
from jax.sharding import PartitionSpec as P

epsilon = 1e-05
MESH = pl.DeviceIdType.MESH
f32 = jnp.float32
bf16 = jnp.bfloat16


def split(x):
    hi = x.astype(bf16)
    return hi, (x - hi.astype(f32)).astype(bf16)


def mm(a, b):
    return jnp.dot(a, b, preferred_element_type=f32)


def standardize(x):
    centered = x - jnp.mean(x, axis=-1, keepdims=True)
    return centered * lax.rsqrt(jnp.mean(centered * centered, axis=-1, keepdims=True) + epsilon)


def stacked(x):
    hi, lo = split(x)
    return jnp.concatenate([hi, lo, hi], axis=1)


def stacked_rows(w):
    hi, lo = split(w)
    return jnp.concatenate([hi, hi, lo], axis=0)


def kernel(dims, *refs):
    (R, C, S, TP, I, J, IB) = dims
    (x_h, res_h, fst_h, snd_h, flat_h, off_h, sw_h, ex_h, sh_h, gs_h, ct_h, sg_h, mx_h) = refs[:13]
    (pair, mixed_o, mstk, x_o) = refs[13:17]
    (x, res, fst, snd, flat, off, sw, ex, sh, gs, ct, sg, mx) = refs[17:30]
    (rowbuf, colbuf, frep, srep, cstk, wf, wg_hh, wg_l, wsh, grep, l2, r2, vals, ohl, w2,
     part, got, wide, mixbuf, in_sem, send_sem, row_sem, col_sem, psend, precv) = refs[30:]
    r, c = lax.axis_index("row"), lax.axis_index("col")
    lin = r * C + c
    B = S * TP
    CD = flat.shape[0]
    D = fst.shape[0]
    HC = ct.shape[1]
    H = gs.shape[0]
    Z = flat.shape[1]
    FF = sw.shape[1]
    F = fst.shape[1]

    barrier = pltpu.get_barrier_semaphore()
    c_dst = lin // R
    slot = lax.rem(lin, R)
    own = c_dst == c

    def greet(a, b):
        pl.semaphore_signal(barrier, inc=1, device_id=(a, b), device_id_type=MESH)

    copies = []
    for n, (src, dst) in enumerate(zip(
        (x_h, fst_h, snd_h, ct_h, sg_h, gs_h, flat_h, off_h, res_h, sw_h, ex_h, sh_h, mx_h),
        (x, fst, snd, ct, sg, gs, flat, off, res, sw, ex, sh, mx))):
        cp = pltpu.make_async_copy(src, dst, in_sem.at[n])
        cp.start()
        copies.append(cp)
    (cx, cfst, csnd, cct, csg, cgs, cflat, coff, cres, csw, cex, csh, cmx) = copies

    for k in range(1, C):
        greet(r, lax.rem(c + k, C))
    for k in range(1, R):
        greet(lax.rem(r + k, R), c_dst)

    @pl.when(jnp.logical_not(own))
    def _():
        greet(r, c_dst)

    for k in range(R):
        src = c * R + k

        @pl.when(src != lin)
        def _():
            greet(src // C, lax.rem(src, C))

    self_in = jnp.where(own, 1, 0)
    cx.wait()
    pl.semaphore_wait(barrier, (C - 1) + 2 * (R - self_in))

    def row_copy(to, at, n):
        return pltpu.make_async_remote_copy(
            src_ref=x, dst_ref=rowbuf.at[pl.ds(pl.multiple_of(at * B, B), B)],
            send_sem=send_sem.at[n], recv_sem=row_sem.at[at],
            device_id=(r, to), device_id_type=MESH)

    def col_copy(to, at, n):
        return pltpu.make_async_remote_copy(
            src_ref=x, dst_ref=colbuf.at[pl.ds(pl.multiple_of(at * B, B), B)],
            send_sem=send_sem.at[n], recv_sem=col_sem.at[at],
            device_id=(to, c_dst), device_id_type=MESH)

    for k in range(1, R):
        col_copy(lax.rem(r + k, R), slot, C + k).start()

    @pl.when(jnp.logical_not(own))
    def _():
        col_copy(r, slot, C).start()

    for k in range(1, C):
        row_copy(lax.rem(c + k, C), c, k).start()

    mine = x[...]
    x_o[...] = mine
    rowbuf[pl.ds(pl.multiple_of(c * B, B), B), :] = mine

    @pl.when(own)
    def _():
        colbuf[pl.ds(pl.multiple_of(slot * B, B), B), :] = mine

    lane = lax.broadcasted_iota(jnp.int32, (D, CD), 1)
    sub = lax.broadcasted_iota(jnp.int32, (D, CD), 0)
    rep_of = jnp.where(lane // D == sub, 1.0, 0.0).astype(bf16)
    tile_of = jnp.where(lax.rem(lane, D) == sub, 1.0, 0.0).astype(bf16)
    for cp, w, e, out in ((cfst, fst, rep_of, frep), (csnd, snd, tile_of, srep)):
        cp.wait()
        hi, lo = split(w[...].T)
        hi = mm(hi, e).astype(bf16)
        out[0:F, :] = hi
        out[F:2 * F, :] = hi
        out[2 * F:3 * F, :] = mm(lo, e).astype(bf16)
    cct.wait()
    cstk[...] = stacked_rows(ct[...])
    cgs.wait()
    head = lax.broadcasted_iota(jnp.int32, (H, HC), 1) // (HC // H)
    spread = jnp.where(head == lax.broadcasted_iota(jnp.int32, (H, HC), 0), 1.0, 0.0).astype(f32)
    grep[...] = jnp.dot(gs[...].T, spread, precision=lax.Precision.HIGHEST, preferred_element_type=f32)
    cflat.wait()
    hi, lo = split(flat[...])
    wf[:, 0:Z] = hi
    wf[:, Z:2 * Z] = lo
    for cp, w, at in ((csw, sw, 0), (cex, ex, FF)):
        cp.wait()
        hi, lo = split(w[...])
        wg_hh[0:Z, at:at + FF] = hi
        wg_hh[Z:2 * Z, at:at + FF] = hi
        wg_l[:, at:at + FF] = lo
    csh.wait()
    hi, lo = split(sh[...])
    wsh[:, 0:Z] = hi
    wsh[:, Z:2 * Z] = lo
    cmx.wait()
    mstk[...] = stacked_rows(mx[...].T)
    csg.wait()
    gate = jax.nn.sigmoid(mm(stacked(standardize(mine)), stacked_rows(sg[...])))

    for k in range(C):
        @pl.when(k != c)
        def _():
            row_copy(c, k, 0).wait_recv()
    l2[...] = mm(stacked(standardize(rowbuf[...])), frep[...]) * (1.0 / S)
    for k in range(R):
        @pl.when(c * R + k != lin)
        def _():
            col_copy(r, k, 0).wait_recv()
    cols = standardize(colbuf[...])
    wide[...] = jnp.concatenate([cols, jnp.zeros((R * B, wide.shape[1] - F), f32)], axis=1)
    cols = jnp.concatenate(
        [wide[pl.ds(s * TP + t, R, stride=B), :] for s in range(S) for t in range(TP)], axis=0)
    cols = stacked(cols[:, 0:F])
    r2[...] = mm(cols, srep[...])
    values = mm(cols, cstk[...])
    for h in range(HC // 128):
        vals[h] = values[:, h * 128:(h + 1) * 128]
    coff.wait()
    cres.wait()

    NP = IB * J

    def chunk(i0):
        if I == IB:
            l2c, resc, pairc = l2, res, pair
        else:
            l2c = l2.at[pl.ds(pl.multiple_of((i0 // TP) * B, B), (IB // TP) * B)]
            rows = pl.ds(pl.multiple_of(i0 * J, IB * J), IB * J)
            resc, pairc = res.at[rows], pair.at[rows]

        def lanes_step(lt, carry):
            at = pl.ds(pl.multiple_of(lt * 128, 128), 128)
            acc = [None] * IB
            for s in range(S):
                right = r2[s * J:(s + 1) * J, at]
                for ii in range(IB):
                    left = l2c[pl.ds((ii // TP) * B + s * TP + ii % TP, 1), at]
                    term = left * right
                    acc[ii] = term if s == 0 else acc[ii] + term
            for ii in range(IB):
                hi, lo = split(acc[ii])
                ohl[ii * J:(ii + 1) * J, at] = hi
                ohl[NP + ii * J:NP + (ii + 1) * J, at] = lo
            return carry

        lax.fori_loop(0, CD // 128, lanes_step, 0)
        up = mm(ohl[...], wf[...])
        update = up[0:NP, 0:Z] + (up[NP:, 0:Z] + up[0:NP, Z:])
        base = jnp.concatenate(
            [resc[pl.ds(ii * J + t, R, stride=TP), :] for ii in range(IB) for t in range(TP)], axis=0)
        mid = base + (update + off[...])
        hi, lo = split(standardize(mid))
        hid = mm(jnp.concatenate([hi, lo], axis=1), wg_hh[...]) + mm(hi, wg_l[...])
        g = hid[:, 0:FF]
        hidden = g / (1.0 + jnp.exp(-g)) * hid[:, FF:]
        hi, lo = split(hidden)
        down = mm(jnp.concatenate([hi, lo], axis=0), wsh[...])
        new = mid + (down[0:NP, 0:Z] + (down[NP:, 0:Z] + down[0:NP, Z:]))
        for ii in range(IB):
            for t in range(TP):
                a = (ii * TP + t) * R
                pairc[pl.ds(ii * J + t, R, stride=TP), :] = new[a:a + R, :]
        logits = jnp.dot(standardize(new), grep[...], precision=lax.Precision.HIGHEST,
                         preferred_element_type=f32)
        for ii in range(IB):
            i = i0 + ii
            row = logits[ii * J:(ii + 1) * J, :]
            peak = jnp.max(row, axis=0, keepdims=True)
            e = jnp.exp(row - peak)
            w2[ii * J:(ii + 1) * J, :] = e
            total = jnp.sum(e, axis=0, keepdims=True)
            which = lax.broadcasted_iota(jnp.int32, (8, HC), 0)
            part[i, S:S + 8, :] = jnp.where(which == 0, total, peak)
        for ii in range(IB):
            for h in range(HC // 128):
                at = slice(h * 128, (h + 1) * 128)
                acc = None
                for j in range(J):
                    term = w2[pl.ds(ii * J + j, 1), at] * vals[h, pl.ds(j, S, stride=J), :]
                    acc = term if acc is None else acc + term
                part[i0 + ii, 0:S, at] = acc

    if I == IB:
        chunk(0)
    else:
        def step(n, carry):
            chunk(n * IB)
            return carry
        lax.fori_loop(0, I // IB, step, 0)

    def part_copy(to, at, n):
        return pltpu.make_async_remote_copy(
            src_ref=part.at[pl.ds(to * TP, TP)], dst_ref=got.at[pl.ds(at * TP, TP)],
            send_sem=psend.at[n], recv_sem=precv.at[at],
            device_id=(r, to), device_id_type=MESH)

    for k in range(1, C):
        part_copy(lax.rem(c + k, C), c, k).start()
    got[pl.ds(c * TP, TP)] = part[pl.ds(c * TP, TP)]

    for k in range(1, R):
        col_copy(lax.rem(r + k, R), slot, C + k).wait_send()

    @pl.when(jnp.logical_not(own))
    def _():
        col_copy(r, slot, C).wait_send()

    for k in range(1, C):
        row_copy(lax.rem(c + k, C), c, k).wait_send()

    for k in range(C):
        @pl.when(k != c)
        def _():
            part_copy(c, k, 0).wait_recv()

    for t in range(TP):
        peaks = [got[k * TP + t, S + 1:S + 2, :] for k in range(C)]
        top = functools.reduce(jnp.maximum, peaks)
        scale = [jnp.exp(p - top) for p in peaks]
        total = sum(got[k * TP + t, S:S + 1, :] * scale[k] for k in range(C))
        summed = sum(got[k * TP + t, 0:S, :] * scale[k] for k in range(C))
        summed = summed / total
        for h in range(HC // 128):
            mixbuf[h, pl.ds(t, S, stride=TP), :] = summed[:, h * 128:(h + 1) * 128]
    mixed_o[...] = gate * jnp.concatenate([mixbuf[h] for h in range(HC // 128)], axis=1)
    for k in range(1, C):
        part_copy(lax.rem(c + k, C), c, k).wait_send()


def finish(pair, mixed, mstk, x, pair_h, hom_o, sem):
    out = pltpu.make_async_copy(pair, pair_h, sem)
    out.start()
    hom_o[...] = x[...] + mm(stacked(mixed[...]), mstk[...])
    out.wait()


def on_device(R, C, homolog_stack, residue_grid, first, second, flatten, offset, switch, expand,
              shrink, score, content, sig, mixing):
    S, TP, F = homolog_stack.shape
    I, J, Z = residue_grid.shape
    IB = max(TP, min(I, 128 // J))
    NP = IB * J
    CD = flatten.shape[0]
    FF = switch.shape[1]
    HC = content.shape[1]
    B = S * TP
    args = (homolog_stack.reshape(B, F), residue_grid.reshape(I * J, Z), first.T, second.T, flatten,
            offset.reshape(1, Z), switch, expand, shrink, score.T, content, sig, mixing.T)
    args = tuple(pltpu.with_memory_space_constraint(a, pltpu.HBM) for a in args)
    dma = pltpu.SemaphoreType.DMA
    pair, mixed, mstk, kept = pl.pallas_call(
        functools.partial(kernel, (R, C, S, TP, I, J, IB)),
        out_shape=(jax.ShapeDtypeStruct((I * J, Z), f32), jax.ShapeDtypeStruct((B, HC), f32),
                   jax.ShapeDtypeStruct((3 * HC, F), bf16), jax.ShapeDtypeStruct((B, F), f32)),
        in_specs=[pl.BlockSpec(memory_space=pltpu.HBM)] * 13,
        out_specs=[pl.BlockSpec(memory_space=pltpu.VMEM)] * 4,
        scratch_shapes=[pltpu.VMEM(a.shape, f32) for a in args] + [
            pltpu.VMEM((C * B, F), f32),
            pltpu.VMEM((R * B, F), f32),
            pltpu.VMEM((3 * F, CD), bf16),
            pltpu.VMEM((3 * F, CD), bf16),
            pltpu.VMEM((3 * F, HC), bf16),
            pltpu.VMEM((CD, 2 * Z), bf16),
            pltpu.VMEM((2 * Z, 2 * FF), bf16),
            pltpu.VMEM((Z, 2 * FF), bf16),
            pltpu.VMEM((FF, 2 * Z), bf16),
            pltpu.VMEM((Z, HC), f32),
            pltpu.VMEM((C * B, CD), f32),
            pltpu.VMEM((S * J, CD), f32),
            pltpu.VMEM((HC // 128, S * J, 128), f32),
            pltpu.VMEM((2 * NP, CD), bf16),
            pltpu.VMEM((NP, HC), f32),
            pltpu.VMEM((I, S + 8, HC), f32),
            pltpu.VMEM((I, S + 8, HC), f32),
            pltpu.VMEM((R * B, 128), f32),
            pltpu.VMEM((HC // 128, B, 128), f32),
            dma((13,)), dma((C + R,)), dma((C,)), dma((R,)), dma((C,)), dma((C,)),
        ],
        compiler_params=pltpu.CompilerParams(
            collective_id=0, has_side_effects=True, vmem_limit_bytes=32 * 1024 * 1024),
        name="msa_block",
    )(*args)
    pair, hom = pl.pallas_call(
        finish,
        out_shape=(jax.ShapeDtypeStruct((I * J, Z), f32), jax.ShapeDtypeStruct((B, F), f32)),
        in_specs=[pl.BlockSpec(memory_space=pltpu.VMEM)] * 4,
        out_specs=(pl.BlockSpec(memory_space=pltpu.HBM), pl.BlockSpec(memory_space=pltpu.VMEM)),
        scratch_shapes=[dma(())],
        compiler_params=pltpu.CompilerParams(vmem_limit_bytes=16 * 1024 * 1024),
        name="msa_finish",
    )(pair, mixed, mstk, kept)
    return pair.reshape(I, J, Z), hom.reshape(S, TP, F)


def solution(mesh):
    R, C = mesh.shape["row"], mesh.shape["col"]
    return jax.shard_map(
        functools.partial(on_device, R, C),
        mesh=mesh,
        in_specs=(P(None, ("row", "col"), None), P("row", "col", None)) + (P(),) * 11,
        out_specs=(P("row", "col", None), P(None, ("row", "col"), None)),
        check_vma=False,
    )
```

```python
import functools

import jax
import jax.numpy as jnp
from jax import lax
from jax.experimental import pallas as pl
from jax.experimental.pallas import tpu as pltpu
from jax.sharding import PartitionSpec as P

epsilon = 1e-05
MESH = pl.DeviceIdType.MESH
f32 = jnp.float32
bf16 = jnp.bfloat16


def split(x):
    hi = x.astype(bf16)
    return hi, (x - hi.astype(f32)).astype(bf16)


def mm(a, b):
    return jnp.dot(a, b, preferred_element_type=f32)


def standardize(x):
    centered = x - jnp.mean(x, axis=-1, keepdims=True)
    return centered * lax.rsqrt(jnp.mean(centered * centered, axis=-1, keepdims=True) + epsilon)


def stacked(x):
    hi, lo = split(x)
    return jnp.concatenate([hi, lo, hi], axis=1)


def stacked_rows(w):
    hi, lo = split(w)
    return jnp.concatenate([hi, hi, lo], axis=0)


def kernel(dims, *refs):
    (R, C, S, TP, I, J, IB) = dims
    (x_h, res_h, fst_h, snd_h, flat_h, off_h, sw_h, ex_h, sh_h, gs_h, ct_h, sg_h, mx_h) = refs[:13]
    (pair, mixed_o, mstk, x_o) = refs[13:17]
    (x, res, fst, snd, flat, off, sw, ex, sh, gs, ct, sg, mx) = refs[17:30]
    (rowbuf, colbuf, frep, srep, cstk, wf, wg_hh, wg_l, wsh, grep, l2, r2, vals, ohl, w2,
     part, stat, got, got_stat, wide, packed, mixbuf, in_sem, send_sem, row_sem, col_sem, psend, precv, ssend, srecv) = refs[30:]
    r, c = lax.axis_index("row"), lax.axis_index("col")
    lin = r * C + c
    B = S * TP
    CD = flat.shape[0]
    D = fst.shape[0]
    HC = ct.shape[1]
    H = gs.shape[0]
    Z = flat.shape[1]
    FF = sw.shape[1]
    F = fst.shape[1]

    barrier = pltpu.get_barrier_semaphore()
    c_dst = lin // R
    slot = lax.rem(lin, R)
    own = c_dst == c

    def greet(a, b):
        pl.semaphore_signal(barrier, inc=1, device_id=(a, b), device_id_type=MESH)

    copies = []
    for n, (src, dst) in enumerate(zip(
        (x_h, fst_h, snd_h, ct_h, sg_h, gs_h, flat_h, off_h, res_h, sw_h, ex_h, sh_h, mx_h),
        (x, fst, snd, ct, sg, gs, flat, off, res, sw, ex, sh, mx))):
        cp = pltpu.make_async_copy(src, dst, in_sem.at[n])
        cp.start()
        copies.append(cp)
    (cx, cfst, csnd, cct, csg, cgs, cflat, coff, cres, csw, cex, csh, cmx) = copies

    for k in range(1, C):
        greet(r, lax.rem(c + k, C))
    for k in range(1, R):
        greet(lax.rem(r + k, R), c_dst)

    @pl.when(jnp.logical_not(own))
    def _():
        greet(r, c_dst)

    for k in range(R):
        src = c * R + k

        @pl.when(src != lin)
        def _():
            greet(src // C, lax.rem(src, C))

    self_in = jnp.where(own, 1, 0)
    cx.wait()
    wide[...] = jnp.concatenate([x[...], jnp.zeros((B, 128 - F), f32)], axis=1)
    packed[...] = jnp.concatenate([wide[pl.ds(t, S, stride=TP), :][:, 0:F] for t in range(TP)], axis=1)
    pl.semaphore_wait(barrier, (C - 1) + 2 * (R - self_in))

    def row_copy(to, at, n):
        return pltpu.make_async_remote_copy(
            src_ref=packed, dst_ref=rowbuf.at[pl.ds(pl.multiple_of(at * S, S), S)],
            send_sem=send_sem.at[n], recv_sem=row_sem.at[at],
            device_id=(r, to), device_id_type=MESH)

    def col_copy(to, at, n):
        return pltpu.make_async_remote_copy(
            src_ref=packed, dst_ref=colbuf.at[pl.ds(pl.multiple_of(at * S, S), S)],
            send_sem=send_sem.at[n], recv_sem=col_sem.at[at],
            device_id=(to, c_dst), device_id_type=MESH)

    for k in range(1, R):
        col_copy(lax.rem(r + k, R), slot, C + k).start()

    @pl.when(jnp.logical_not(own))
    def _():
        col_copy(r, slot, C).start()

    for k in range(1, C):
        row_copy(lax.rem(c + k, C), c, k).start()

    mine = x[...]
    x_o[...] = mine
    rowbuf[pl.ds(pl.multiple_of(c * S, S), S), :] = packed[...]

    @pl.when(own)
    def _():
        colbuf[pl.ds(pl.multiple_of(slot * S, S), S), :] = packed[...]

    lane = lax.broadcasted_iota(jnp.int32, (D, CD), 1)
    sub = lax.broadcasted_iota(jnp.int32, (D, CD), 0)
    rep_of = jnp.where(lane // D == sub, 1.0, 0.0).astype(bf16)
    tile_of = jnp.where(lax.rem(lane, D) == sub, 1.0, 0.0).astype(bf16)
    for cp, w, e, out in ((cfst, fst, rep_of, frep), (csnd, snd, tile_of, srep)):
        cp.wait()
        hi, lo = split(w[...].T)
        hi = mm(hi, e).astype(bf16)
        out[0:F, :] = hi
        out[F:2 * F, :] = hi
        out[2 * F:3 * F, :] = mm(lo, e).astype(bf16)
    cct.wait()
    cstk[...] = stacked_rows(ct[...])
    cgs.wait()
    head = lax.broadcasted_iota(jnp.int32, (H, HC), 1) // (HC // H)
    spread = jnp.where(head == lax.broadcasted_iota(jnp.int32, (H, HC), 0), 1.0, 0.0).astype(f32)
    grep[...] = jnp.dot(gs[...].T, spread, precision=lax.Precision.HIGHEST, preferred_element_type=f32)
    cflat.wait()
    hi, lo = split(flat[...])
    wf[:, 0:Z] = hi
    wf[:, Z:2 * Z] = lo
    for cp, w, at in ((csw, sw, 0), (cex, ex, FF)):
        cp.wait()
        hi, lo = split(w[...])
        wg_hh[0:Z, at:at + FF] = hi
        wg_hh[Z:2 * Z, at:at + FF] = hi
        wg_l[:, at:at + FF] = lo
    csh.wait()
    hi, lo = split(sh[...])
    wsh[:, 0:Z] = hi
    wsh[:, Z:2 * Z] = lo
    cmx.wait()
    mstk[...] = stacked_rows(mx[...].T)
    csg.wait()
    gate = jax.nn.sigmoid(mm(stacked(standardize(mine)), stacked_rows(sg[...])))

    for k in range(C):
        @pl.when(k != c)
        def _():
            row_copy(c, k, 0).wait_recv()

    def tokens(block):
        return jnp.concatenate([standardize(block[:, t * F:(t + 1) * F]) for t in range(TP)], axis=0)

    l2[...] = mm(stacked(tokens(rowbuf[...])), frep[...]) * (1.0 / S)
    for k in range(R):
        @pl.when(c * R + k != lin)
        def _():
            col_copy(r, k, 0).wait_recv()
    cols = stacked(tokens(jnp.concatenate(
        [colbuf[pl.ds(s, R, stride=S), :] for s in range(S)], axis=0)))
    r2[...] = mm(cols, srep[...])
    values = mm(cols, cstk[...])
    for h in range(HC // 128):
        vals[h] = values[:, h * 128:(h + 1) * 128]
    coff.wait()
    cres.wait()

    NP = IB * J

    def part_copy(to, at):
        return pltpu.make_async_remote_copy(
            src_ref=part.at[pl.ds(to * TP, TP)], dst_ref=got.at[pl.ds(at * TP, TP)],
            send_sem=psend.at[to], recv_sem=precv.at[at],
            device_id=(r, to), device_id_type=MESH)

    def stat_copy(to, at):
        return pltpu.make_async_remote_copy(
            src_ref=stat.at[to], dst_ref=got_stat.at[at],
            send_sem=ssend.at[to], recv_sem=srecv.at[at],
            device_id=(r, to), device_id_type=MESH)

    def chunk(i0):
        d0 = i0 // TP
        l2c = [l2.at[pl.ds(pl.multiple_of((t * C + d0) * S, S), (IB // TP) * S)] for t in range(TP)]
        rows = pl.ds(pl.multiple_of(i0 * J, IB * J), IB * J)
        resc, pairc = res.at[rows], pair.at[rows]

        def lanes_step(lt, carry):
            at = pl.ds(pl.multiple_of(lt * 128, 128), 128)
            acc = [None] * IB
            for s in range(S):
                right = jnp.concatenate(
                    [r2[(t * S + s) * R:(t * S + s + 1) * R, at] for t in range(TP)], axis=0)
                for ii in range(IB):
                    left = l2c[ii % TP][pl.ds((ii // TP) * S + s, 1), at]
                    term = left * right
                    acc[ii] = term if s == 0 else acc[ii] + term
            for ii in range(IB):
                hi, lo = split(acc[ii])
                ohl[ii * J:(ii + 1) * J, at] = hi
                ohl[NP + ii * J:NP + (ii + 1) * J, at] = lo
            return carry

        lax.fori_loop(0, CD // 128, lanes_step, 0)
        up = mm(ohl[...], wf[...])
        update = up[0:NP, 0:Z] + (up[NP:, 0:Z] + up[0:NP, Z:])
        base = jnp.concatenate(
            [resc[pl.ds(ii * J + t, R, stride=TP), :] for ii in range(IB) for t in range(TP)], axis=0)
        mid = base + (update + off[...])
        hi, lo = split(standardize(mid))
        hid = mm(jnp.concatenate([hi, lo], axis=1), wg_hh[...]) + mm(hi, wg_l[...])
        g = hid[:, 0:FF]
        hidden = g / (1.0 + jnp.exp(-g)) * hid[:, FF:]
        hi, lo = split(hidden)
        down = mm(jnp.concatenate([hi, lo], axis=0), wsh[...])
        new = mid + (down[0:NP, 0:Z] + (down[NP:, 0:Z] + down[0:NP, Z:]))
        for ii in range(IB):
            for t in range(TP):
                a = (ii * TP + t) * R
                pairc[pl.ds(ii * J + t, R, stride=TP), :] = new[a:a + R, :]
        logits = jnp.dot(standardize(new), grep[...], precision=lax.Precision.HIGHEST,
                         preferred_element_type=f32)
        for d in range(IB // TP):
            notes = []
            for t in range(TP):
                ii = d * TP + t
                row = logits[ii * J:(ii + 1) * J, :]
                peak = jnp.max(row, axis=0, keepdims=True)
                e = jnp.exp(row - peak)
                w2[ii * J:(ii + 1) * J, :] = e
                notes += [jnp.sum(e, axis=0, keepdims=True), peak]
            notes.append(jnp.zeros((8 - 2 * TP, HC), f32))
            stat[d0 + d] = jnp.concatenate(notes, axis=0)
        for ii in range(IB):
            for h in range(HC // 128):
                at = slice(h * 128, (h + 1) * 128)
                acc = None
                for j in range(J):
                    term = w2[pl.ds(ii * J + j, 1), at] * vals[h, pl.ds((j // R) * S * R + j % R, S, stride=R), :]
                    acc = term if acc is None else acc + term
                part[i0 + ii, :, at] = acc
        for d in range(IB // TP):
            @pl.when(d0 + d != c)
            def _():
                part_copy(d0 + d, c).start()
                stat_copy(d0 + d, c).start()

    count = I // IB
    last = (c * TP) // IB
    if count <= 2:
        for n in range(count):
            chunk(lax.rem(last + 1 + n, count) * IB)
    else:
        def step(n, carry):
            chunk(lax.rem(last + 1 + n, count) * IB)
            return carry
        lax.fori_loop(0, count, step, 0)

    got[pl.ds(c * TP, TP)] = part[pl.ds(c * TP, TP)]
    got_stat[c] = stat[c]

    for k in range(1, R):
        col_copy(lax.rem(r + k, R), slot, C + k).wait_send()

    @pl.when(jnp.logical_not(own))
    def _():
        col_copy(r, slot, C).wait_send()

    for k in range(1, C):
        row_copy(lax.rem(c + k, C), c, k).wait_send()

    for k in range(C):
        @pl.when(k != c)
        def _():
            part_copy(c, k).wait_recv()
            stat_copy(c, k).wait_recv()

    for t in range(TP):
        peaks = [got_stat[k, 2 * t + 1:2 * t + 2, :] for k in range(C)]
        top = functools.reduce(jnp.maximum, peaks)
        scale = [jnp.exp(p - top) for p in peaks]
        total = sum(got_stat[k, 2 * t:2 * t + 1, :] * scale[k] for k in range(C))
        summed = sum(got[k * TP + t] * scale[k] for k in range(C))
        summed = summed / total
        for h in range(HC // 128):
            mixbuf[h, pl.ds(t, S, stride=TP), :] = summed[:, h * 128:(h + 1) * 128]
    mixed_o[...] = gate * jnp.concatenate([mixbuf[h] for h in range(HC // 128)], axis=1)
    for k in range(1, C):
        part_copy(lax.rem(c + k, C), c).wait_send()
        stat_copy(lax.rem(c + k, C), c).wait_send()


def finish(pair, mixed, mstk, x, pair_h, hom_o, sem):
    out = pltpu.make_async_copy(pair, pair_h, sem)
    out.start()
    hom_o[...] = x[...] + mm(stacked(mixed[...]), mstk[...])
    out.wait()


def on_device(R, C, homolog_stack, residue_grid, first, second, flatten, offset, switch, expand,
              shrink, score, content, sig, mixing):
    S, TP, F = homolog_stack.shape
    I, J, Z = residue_grid.shape
    IB = max(TP, min(I // 2, 64 // J))
    NP = IB * J
    CD = flatten.shape[0]
    FF = switch.shape[1]
    HC = content.shape[1]
    B = S * TP
    args = (homolog_stack.reshape(B, F), residue_grid.reshape(I * J, Z), first.T, second.T, flatten,
            offset.reshape(1, Z), switch, expand, shrink, score.T, content, sig, mixing.T)
    args = tuple(pltpu.with_memory_space_constraint(a, pltpu.HBM) for a in args)
    dma = pltpu.SemaphoreType.DMA
    pair, mixed, mstk, kept = pl.pallas_call(
        functools.partial(kernel, (R, C, S, TP, I, J, IB)),
        out_shape=(jax.ShapeDtypeStruct((I * J, Z), f32), jax.ShapeDtypeStruct((B, HC), f32),
                   jax.ShapeDtypeStruct((3 * HC, F), bf16), jax.ShapeDtypeStruct((B, F), f32)),
        in_specs=[pl.BlockSpec(memory_space=pltpu.HBM)] * 13,
        out_specs=[pl.BlockSpec(memory_space=pltpu.VMEM)] * 4,
        scratch_shapes=[pltpu.VMEM(a.shape, f32) for a in args] + [
            pltpu.VMEM((C * S, TP * F), f32),
            pltpu.VMEM((R * S, TP * F), f32),
            pltpu.VMEM((3 * F, CD), bf16),
            pltpu.VMEM((3 * F, CD), bf16),
            pltpu.VMEM((3 * F, HC), bf16),
            pltpu.VMEM((CD, 2 * Z), bf16),
            pltpu.VMEM((2 * Z, 2 * FF), bf16),
            pltpu.VMEM((Z, 2 * FF), bf16),
            pltpu.VMEM((FF, 2 * Z), bf16),
            pltpu.VMEM((Z, HC), f32),
            pltpu.VMEM((C * B, CD), f32),
            pltpu.VMEM((S * J, CD), f32),
            pltpu.VMEM((HC // 128, S * J, 128), f32),
            pltpu.VMEM((2 * NP, CD), bf16),
            pltpu.VMEM((NP, HC), f32),
            pltpu.VMEM((I, S, HC), f32),
            pltpu.VMEM((C, 8, HC), f32),
            pltpu.VMEM((I, S, HC), f32),
            pltpu.VMEM((C, 8, HC), f32),
            pltpu.VMEM((B, 128), f32),
            pltpu.VMEM((S, TP * F), f32),
            pltpu.VMEM((HC // 128, B, 128), f32),
            dma((13,)), dma((C + R,)), dma((C,)), dma((R,)), dma((C,)), dma((C,)), dma((C,)), dma((C,)),
        ],
        compiler_params=pltpu.CompilerParams(
            collective_id=0, has_side_effects=True, vmem_limit_bytes=32 * 1024 * 1024),
        name="msa_block",
    )(*args)
    pair, hom = pl.pallas_call(
        finish,
        out_shape=(jax.ShapeDtypeStruct((I * J, Z), f32), jax.ShapeDtypeStruct((B, F), f32)),
        in_specs=[pl.BlockSpec(memory_space=pltpu.VMEM)] * 4,
        out_specs=(pl.BlockSpec(memory_space=pltpu.HBM), pl.BlockSpec(memory_space=pltpu.VMEM)),
        scratch_shapes=[dma(())],
        compiler_params=pltpu.CompilerParams(vmem_limit_bytes=16 * 1024 * 1024),
        name="msa_finish",
    )(pair, mixed, mstk, kept)
    return pair.reshape(I, J, Z), hom.reshape(S, TP, F)


def solution(mesh):
    R, C = mesh.shape["row"], mesh.shape["col"]
    return jax.shard_map(
        functools.partial(on_device, R, C),
        mesh=mesh,
        in_specs=(P(None, ("row", "col"), None), P("row", "col", None)) + (P(),) * 11,
        out_specs=(P("row", "col", None), P(None, ("row", "col"), None)),
        check_vma=False,
    )
```

```python
import functools

import jax
import jax.numpy as jnp
from jax import lax
from jax.experimental import pallas as pl
from jax.experimental.pallas import tpu as pltpu
from jax.sharding import PartitionSpec as P

epsilon = 1e-05
MESH = pl.DeviceIdType.MESH
f32 = jnp.float32
bf16 = jnp.bfloat16


def split(x):
    hi = x.astype(bf16)
    return hi, (x - hi.astype(f32)).astype(bf16)


def mm(a, b):
    return jnp.dot(a, b, preferred_element_type=f32)


def standardize(x):
    centered = x - jnp.mean(x, axis=-1, keepdims=True)
    return centered * lax.rsqrt(jnp.mean(centered * centered, axis=-1, keepdims=True) + epsilon)


def stacked(x):
    hi, lo = split(x)
    return jnp.concatenate([hi, lo, hi], axis=1)


def stacked_rows(w):
    hi, lo = split(w)
    return jnp.concatenate([hi, hi, lo], axis=0)


def kernel(dims, *refs):
    (R, C, S, TP, I, J, IB) = dims
    (x_h, res_h, fst_h, snd_h, flat_h, off_h, sw_h, ex_h, sh_h, gs_h, ct_h, sg_h, mx_h) = refs[:13]
    (pair, mixed_o, mstk, x_o) = refs[13:17]
    (x, res, fst, snd, flat, off, sw, ex, sh, gs, ct, sg, mx) = refs[17:30]
    (rowbuf, colbuf, frep, srep, cstk, wf, wg_hh, wg_l, wsh, grep, l2, r2, vals, ohl, w2,
     part, stat, got, got_stat, wide, packed, mixbuf, in_sem, send_sem, row_sem, col_sem, psend, precv, ssend, srecv) = refs[30:]
    r, c = lax.axis_index("row"), lax.axis_index("col")
    lin = r * C + c
    B = S * TP
    CD = flat.shape[0]
    D = fst.shape[0]
    HC = ct.shape[1]
    H = gs.shape[0]
    Z = flat.shape[1]
    FF = sw.shape[1]
    F = fst.shape[1]

    barrier = pltpu.get_barrier_semaphore()
    c_dst = lin // R
    slot = lax.rem(lin, R)
    own = c_dst == c

    def greet(a, b):
        pl.semaphore_signal(barrier, inc=1, device_id=(a, b), device_id_type=MESH)

    copies = []
    for n, (src, dst) in enumerate(zip(
        (x_h, fst_h, snd_h, ct_h, sg_h, gs_h, flat_h, off_h, res_h, sw_h, ex_h, sh_h, mx_h),
        (x, fst, snd, ct, sg, gs, flat, off, res, sw, ex, sh, mx))):
        cp = pltpu.make_async_copy(src, dst, in_sem.at[n])
        cp.start()
        copies.append(cp)
    (cx, cfst, csnd, cct, csg, cgs, cflat, coff, cres, csw, cex, csh, cmx) = copies

    for k in range(1, C):
        greet(r, lax.rem(c + k, C))
    for k in range(1, R):
        greet(lax.rem(r + k, R), c_dst)

    @pl.when(jnp.logical_not(own))
    def _():
        greet(r, c_dst)

    for k in range(R):
        src = c * R + k

        @pl.when(src != lin)
        def _():
            greet(src // C, lax.rem(src, C))

    self_in = jnp.where(own, 1, 0)
    cx.wait()
    wide[...] = jnp.concatenate([x[...], jnp.zeros((B, 128 - F), f32)], axis=1)
    packed[...] = jnp.concatenate([wide[pl.ds(t, S, stride=TP), :][:, 0:F] for t in range(TP)], axis=1)
    pl.semaphore_wait(barrier, (C - 1) + 2 * (R - self_in))

    def row_copy(to, at, n):
        return pltpu.make_async_remote_copy(
            src_ref=packed, dst_ref=rowbuf.at[pl.ds(pl.multiple_of(at * S, S), S)],
            send_sem=send_sem.at[n], recv_sem=row_sem.at[at],
            device_id=(r, to), device_id_type=MESH)

    def col_copy(to, at, n):
        return pltpu.make_async_remote_copy(
            src_ref=packed, dst_ref=colbuf.at[pl.ds(pl.multiple_of(at * S, S), S)],
            send_sem=send_sem.at[n], recv_sem=col_sem.at[at],
            device_id=(to, c_dst), device_id_type=MESH)

    for k in range(1, R):
        col_copy(lax.rem(r + k, R), slot, C + k).start()

    @pl.when(jnp.logical_not(own))
    def _():
        col_copy(r, slot, C).start()

    for k in range(1, C):
        row_copy(lax.rem(c + k, C), c, k).start()

    mine = x[...]
    x_o[...] = mine
    rowbuf[pl.ds(pl.multiple_of(c * S, S), S), :] = packed[...]

    @pl.when(own)
    def _():
        colbuf[pl.ds(pl.multiple_of(slot * S, S), S), :] = packed[...]

    lane = lax.broadcasted_iota(jnp.int32, (D, CD), 1)
    sub = lax.broadcasted_iota(jnp.int32, (D, CD), 0)
    rep_of = jnp.where(lane // D == sub, 1.0, 0.0).astype(bf16)
    tile_of = jnp.where(lax.rem(lane, D) == sub, 1.0, 0.0).astype(bf16)
    for cp, w, e, out in ((cfst, fst, rep_of, frep), (csnd, snd, tile_of, srep)):
        cp.wait()
        hi, lo = split(w[...].T)
        hi = mm(hi, e).astype(bf16)
        out[0:F, :] = hi
        out[F:2 * F, :] = hi
        out[2 * F:3 * F, :] = mm(lo, e).astype(bf16)
    cct.wait()
    cstk[...] = stacked_rows(ct[...])
    cgs.wait()
    head = lax.broadcasted_iota(jnp.int32, (H, HC), 1) // (HC // H)
    spread = jnp.where(head == lax.broadcasted_iota(jnp.int32, (H, HC), 0), 1.0, 0.0).astype(f32)
    grep[...] = jnp.dot(gs[...].T, spread, precision=lax.Precision.HIGHEST, preferred_element_type=f32)
    cflat.wait()
    hi, lo = split(flat[...])
    wf[:, 0:Z] = hi
    wf[:, Z:2 * Z] = lo
    for cp, w, at in ((csw, sw, 0), (cex, ex, FF)):
        cp.wait()
        hi, lo = split(w[...])
        wg_hh[0:Z, at:at + FF] = hi
        wg_hh[Z:2 * Z, at:at + FF] = hi
        wg_l[:, at:at + FF] = lo
    csh.wait()
    hi, lo = split(sh[...])
    wsh[:, 0:Z] = hi
    wsh[:, Z:2 * Z] = lo
    cmx.wait()
    mstk[...] = stacked_rows(mx[...].T)
    csg.wait()
    gate = jax.nn.sigmoid(mm(stacked(standardize(mine)), stacked_rows(sg[...])))

    for k in range(C):
        @pl.when(k != c)
        def _():
            row_copy(c, k, 0).wait_recv()

    def tokens(block):
        return jnp.concatenate([standardize(block[:, t * F:(t + 1) * F]) for t in range(TP)], axis=0)

    l2[...] = mm(stacked(tokens(rowbuf[...])), frep[...]) * (1.0 / S)
    for k in range(R):
        @pl.when(c * R + k != lin)
        def _():
            col_copy(r, k, 0).wait_recv()
    cols = stacked(tokens(jnp.concatenate(
        [colbuf[pl.ds(s, R, stride=S), :] for s in range(S)], axis=0)))
    r2[...] = mm(cols, srep[...])
    values = mm(cols, cstk[...])
    for h in range(HC // 128):
        vals[h] = values[:, h * 128:(h + 1) * 128]
    coff.wait()
    cres.wait()

    NP = IB * J

    def part_copy(to, at):
        return pltpu.make_async_remote_copy(
            src_ref=part.at[pl.ds(to * TP, TP)], dst_ref=got.at[pl.ds(at * TP, TP)],
            send_sem=psend.at[to], recv_sem=precv.at[at],
            device_id=(r, to), device_id_type=MESH)

    def stat_copy(to, at):
        return pltpu.make_async_remote_copy(
            src_ref=stat.at[to], dst_ref=got_stat.at[at],
            send_sem=ssend.at[to], recv_sem=srecv.at[at],
            device_id=(r, to), device_id_type=MESH)

    def chunk(i0):
        d0 = i0 // TP
        l2c = [l2.at[pl.ds(pl.multiple_of((t * C + d0) * S, S), (IB // TP) * S)] for t in range(TP)]
        rows = pl.ds(pl.multiple_of(i0 * J, IB * J), IB * J)
        resc, pairc = res.at[rows], pair.at[rows]

        def lanes_step(lt, carry):
            at = pl.ds(pl.multiple_of(lt * 128, 128), 128)
            acc = [None] * IB
            for s in range(S):
                right = jnp.concatenate(
                    [r2[(t * S + s) * R:(t * S + s + 1) * R, at] for t in range(TP)], axis=0)
                for ii in range(IB):
                    left = l2c[ii % TP][pl.ds((ii // TP) * S + s, 1), at]
                    term = left * right
                    acc[ii] = term if s == 0 else acc[ii] + term
            for ii in range(IB):
                hi, lo = split(acc[ii])
                ohl[ii * J:(ii + 1) * J, at] = hi
                ohl[NP + ii * J:NP + (ii + 1) * J, at] = lo
            return carry

        lax.fori_loop(0, CD // 128, lanes_step, 0, unroll=4)
        up = mm(ohl[...], wf[...])
        update = up[0:NP, 0:Z] + (up[NP:, 0:Z] + up[0:NP, Z:])
        base = jnp.concatenate(
            [resc[pl.ds(ii * J + t, R, stride=TP), :] for ii in range(IB) for t in range(TP)], axis=0)
        mid = base + (update + off[...])
        hi, lo = split(standardize(mid))
        hid = mm(jnp.concatenate([hi, lo], axis=1), wg_hh[...]) + mm(hi, wg_l[...])
        g = hid[:, 0:FF]
        hidden = g / (1.0 + jnp.exp(-g)) * hid[:, FF:]
        hi, lo = split(hidden)
        down = mm(jnp.concatenate([hi, lo], axis=0), wsh[...])
        new = mid + (down[0:NP, 0:Z] + (down[NP:, 0:Z] + down[0:NP, Z:]))
        for ii in range(IB):
            for t in range(TP):
                a = (ii * TP + t) * R
                pairc[pl.ds(ii * J + t, R, stride=TP), :] = new[a:a + R, :]
        logits = jnp.dot(standardize(new), grep[...], precision=lax.Precision.HIGHEST,
                         preferred_element_type=f32)
        for d in range(IB // TP):
            notes = []
            for t in range(TP):
                ii = d * TP + t
                row = logits[ii * J:(ii + 1) * J, :]
                peak = jnp.max(row, axis=0, keepdims=True)
                e = jnp.exp(row - peak)
                w2[ii * J:(ii + 1) * J, :] = e
                notes += [jnp.sum(e, axis=0, keepdims=True), peak]
            notes.append(jnp.zeros((8 - 2 * TP, HC), f32))
            stat[d0 + d] = jnp.concatenate(notes, axis=0)
        for d in range(IB // TP):
            for ii in range(d * TP, (d + 1) * TP):
                for h in range(HC // 128):
                    at = slice(h * 128, (h + 1) * 128)
                    acc = None
                    for j in range(J):
                        term = w2[pl.ds(ii * J + j, 1), at] * vals[h, pl.ds((j // R) * S * R + j % R, S, stride=R), :]
                        acc = term if acc is None else acc + term
                    part[i0 + ii, :, at] = acc

            @pl.when(d0 + d != c)
            def _():
                part_copy(d0 + d, c).start()
                stat_copy(d0 + d, c).start()

    count = I // IB
    last = (c * TP) // IB
    if count <= 2:
        for n in range(count):
            chunk(lax.rem(last + 1 + n, count) * IB)
    else:
        def step(n, carry):
            chunk(lax.rem(last + 1 + n, count) * IB)
            return carry
        lax.fori_loop(0, count, step, 0)

    got[pl.ds(c * TP, TP)] = part[pl.ds(c * TP, TP)]
    got_stat[c] = stat[c]

    for k in range(1, R):
        col_copy(lax.rem(r + k, R), slot, C + k).wait_send()

    @pl.when(jnp.logical_not(own))
    def _():
        col_copy(r, slot, C).wait_send()

    for k in range(1, C):
        row_copy(lax.rem(c + k, C), c, k).wait_send()

    for k in range(C):
        @pl.when(k != c)
        def _():
            part_copy(c, k).wait_recv()
            stat_copy(c, k).wait_recv()

    for t in range(TP):
        peaks = [got_stat[k, 2 * t + 1:2 * t + 2, :] for k in range(C)]
        top = functools.reduce(jnp.maximum, peaks)
        scale = [jnp.exp(p - top) for p in peaks]
        total = sum(got_stat[k, 2 * t:2 * t + 1, :] * scale[k] for k in range(C))
        summed = sum(got[k * TP + t] * scale[k] for k in range(C))
        summed = summed / total
        for h in range(HC // 128):
            mixbuf[h, pl.ds(t, S, stride=TP), :] = summed[:, h * 128:(h + 1) * 128]
    mixed_o[...] = gate * jnp.concatenate([mixbuf[h] for h in range(HC // 128)], axis=1)
    for k in range(1, C):
        part_copy(lax.rem(c + k, C), c).wait_send()
        stat_copy(lax.rem(c + k, C), c).wait_send()


def finish(pair, mixed, mstk, x, pair_h, hom_o, sem):
    out = pltpu.make_async_copy(pair, pair_h, sem)
    out.start()
    hom_o[...] = x[...] + mm(stacked(mixed[...]), mstk[...])
    out.wait()


def on_device(R, C, homolog_stack, residue_grid, first, second, flatten, offset, switch, expand,
              shrink, score, content, sig, mixing):
    S, TP, F = homolog_stack.shape
    I, J, Z = residue_grid.shape
    IB = max(TP, min(I // 2, 64 // J))
    NP = IB * J
    CD = flatten.shape[0]
    FF = switch.shape[1]
    HC = content.shape[1]
    B = S * TP
    args = (homolog_stack.reshape(B, F), residue_grid.reshape(I * J, Z), first.T, second.T, flatten,
            offset.reshape(1, Z), switch, expand, shrink, score.T, content, sig, mixing.T)
    args = tuple(pltpu.with_memory_space_constraint(a, pltpu.HBM) for a in args)
    dma = pltpu.SemaphoreType.DMA
    pair, mixed, mstk, kept = pl.pallas_call(
        functools.partial(kernel, (R, C, S, TP, I, J, IB)),
        out_shape=(jax.ShapeDtypeStruct((I * J, Z), f32), jax.ShapeDtypeStruct((B, HC), f32),
                   jax.ShapeDtypeStruct((3 * HC, F), bf16), jax.ShapeDtypeStruct((B, F), f32)),
        in_specs=[pl.BlockSpec(memory_space=pltpu.HBM)] * 13,
        out_specs=[pl.BlockSpec(memory_space=pltpu.VMEM)] * 4,
        scratch_shapes=[pltpu.VMEM(a.shape, f32) for a in args] + [
            pltpu.VMEM((C * S, TP * F), f32),
            pltpu.VMEM((R * S, TP * F), f32),
            pltpu.VMEM((3 * F, CD), bf16),
            pltpu.VMEM((3 * F, CD), bf16),
            pltpu.VMEM((3 * F, HC), bf16),
            pltpu.VMEM((CD, 2 * Z), bf16),
            pltpu.VMEM((2 * Z, 2 * FF), bf16),
            pltpu.VMEM((Z, 2 * FF), bf16),
            pltpu.VMEM((FF, 2 * Z), bf16),
            pltpu.VMEM((Z, HC), f32),
            pltpu.VMEM((C * B, CD), f32),
            pltpu.VMEM((S * J, CD), f32),
            pltpu.VMEM((HC // 128, S * J, 128), f32),
            pltpu.VMEM((2 * NP, CD), bf16),
            pltpu.VMEM((NP, HC), f32),
            pltpu.VMEM((I, S, HC), f32),
            pltpu.VMEM((C, 8, HC), f32),
            pltpu.VMEM((I, S, HC), f32),
            pltpu.VMEM((C, 8, HC), f32),
            pltpu.VMEM((B, 128), f32),
            pltpu.VMEM((S, TP * F), f32),
            pltpu.VMEM((HC // 128, B, 128), f32),
            dma((13,)), dma((C + R,)), dma((C,)), dma((R,)), dma((C,)), dma((C,)), dma((C,)), dma((C,)),
        ],
        compiler_params=pltpu.CompilerParams(
            collective_id=0, has_side_effects=True, vmem_limit_bytes=32 * 1024 * 1024),
        name="msa_block",
    )(*args)
    pair, hom = pl.pallas_call(
        finish,
        out_shape=(jax.ShapeDtypeStruct((I * J, Z), f32), jax.ShapeDtypeStruct((B, F), f32)),
        in_specs=[pl.BlockSpec(memory_space=pltpu.VMEM)] * 4,
        out_specs=(pl.BlockSpec(memory_space=pltpu.HBM), pl.BlockSpec(memory_space=pltpu.VMEM)),
        scratch_shapes=[dma(())],
        compiler_params=pltpu.CompilerParams(vmem_limit_bytes=16 * 1024 * 1024),
        name="msa_finish",
    )(pair, mixed, mstk, kept)
    return pair.reshape(I, J, Z), hom.reshape(S, TP, F)


def solution(mesh):
    R, C = mesh.shape["row"], mesh.shape["col"]
    return jax.shard_map(
        functools.partial(on_device, R, C),
        mesh=mesh,
        in_specs=(P(None, ("row", "col"), None), P("row", "col", None)) + (P(),) * 11,
        out_specs=(P("row", "col", None), P(None, ("row", "col"), None)),
        check_vma=False,
    )
```
